32 devices in a mesh: pb: 2 (over x), col: 16 (over z, y, core).
Axes of the slice: x: 2, y: 2, z: 4, core: 2. Of those that a mesh axis runs over, the one named last changes fastest.
Arguments:
- queries: bfloat16 [4096, 1024], P(('pb', 'col')), may hold values from -64 to 64
- candidates: bfloat16 [16384, 1024], P(('col', 'pb')), may hold values from -5 to 5
- grades: int32 [4096, 16384], P('pb', 'col'), may hold values from 0 to 4
- query_weights: float32 [4096], P('pb'), may hold values from -0.046875 to 0.046875
Outputs:
- losses: float32 [4096], P('pb')
- query_grad: bfloat16 [4096, 1024], P(('pb', 'col'))
- cand_grad: bfloat16 [16384, 1024], P(('col', 'pb'))
The draws below stay inside these ranges and needn't reach their ends.
All inputs are finite; a program needn't handle non-finite values.
Results may differ from the reference program's by a relative error of at most 0.0071.
Values may be sent and summed in bfloat16 or wider, within the bound.
No kernel may reach another device: no remote copies, remote signals or barrier semaphores. Data moves between devices by JAX's collectives and lax.ppermute only.
A program may use at most 128 MiB of HBM per device.

```python
import math
import jax
import jax.numpy as jnp
from jax import lax

D = 1024
GRADES = 5
NQ = 4096
NC = 16384


def embed_pair(key):
    query_key = jax.random.fold_in(key, 11)
    cand_key = jax.random.fold_in(key, 12)
    candidates = jnp.clip(jax.random.normal(cand_key, (NC, D), jnp.float32), -5.0, 5.0)
    queries = jnp.clip(jax.random.normal(query_key, (NQ, D), jnp.float32), -5.0, 5.0)
    return (queries, candidates)


def draw_queries(key, part):
    queries, candidates = embed_pair(key)
    return queries.astype(jnp.bfloat16)


def draw_candidates(key, part):
    queries, candidates = embed_pair(key)
    return candidates.astype(jnp.bfloat16)


def draw_grades(key, part):
    kind_key = jax.random.fold_in(key, 21)
    single_key = jax.random.fold_in(key, 22)
    cell_key = jax.random.fold_in(key, 23)
    kinds = jax.random.randint(kind_key, (NQ, 1), 0, 16)
    single = jax.random.randint(single_key, (NQ, 1), 0, GRADES)
    cells = jax.random.randint(cell_key, (NQ, NC), 0, 60)
    spread = cells % GRADES
    upper = 1 + cells % 4
    middle = 2 + cells % 2
    lower = cells % 3
    grades = jnp.where(kinds == 0, upper, jnp.where(kinds == 1, middle, jnp.where(kinds == 2, single, jnp.where(kinds == 3, lower, spread))))
    return grades.astype(jnp.int32)


def steps_of(key, dims, split, smallest, high):
    factor_of, own = 1.0, jax.random.fold_in(key, 6)
    for position, shards_of in split:
        heights = jnp.exp(jax.random.uniform(jax.random.fold_in(own, position), (shards_of,), jnp.float32, smallest / len(split), high / len(split)))
        factor_of = factor_of * jnp.repeat(heights, dims[position] // shards_of).reshape([-1 if axis == position else 1 for axis in range(len(dims))])
    return factor_of


def noise(rng, dims, scale, limit, split=(), held_as=jnp.bfloat16):
    result = scale * jax.random.normal(rng, dims, jnp.float32)
    if split:
        result = result * steps_of(rng, dims, split, -0.22, 0.18)
    return jnp.clip(result, -limit, limit).astype(held_as)


def setup_inputs(seed: int = 0) -> dict:
    streams_of = jax.random.split(jax.random.key(seed), 5)
    return {
        "queries": draw_queries(jax.random.fold_in(streams_of[4], 71), 0),
        "candidates": draw_candidates(jax.random.fold_in(streams_of[4], 71), 0),
        "grades": draw_grades(jax.random.fold_in(streams_of[4], 71), 0),
        "query_weights": noise(streams_of[3], (NQ,), NC ** -0.5, 0.046875, ((0, 2),), jnp.float32),
    }


lowest = -1e+30

def grade_levels(maxima, masses, counts):
    levels = []
    running = maxima[0]
    seen_count = counts[0] * 0.0
    for bucket in range(len(maxima)):
        running = jnp.maximum(running, maxima[bucket])
        seen_count = seen_count + counts[bucket]
        summed = masses[0] * jnp.exp(maxima[0] - running)
        for lesser in range(1, bucket + 1):
            summed = summed + masses[lesser] * jnp.exp(maxima[lesser] - running)
        present = seen_count > 0.0
        levels.append(jnp.where(present, running + jnp.log(jnp.where(present, summed, 1.0)), running))
    return levels

def slope_factors(maxima, levels, counts):
    factors = []
    for bucket in range(len(maxima)):
        summed = counts[bucket] * jnp.exp(maxima[bucket] - levels[bucket])
        for higher in range(bucket + 1, len(maxima)):
            summed = summed + counts[higher] * jnp.exp(maxima[bucket] - levels[higher])
        factors.append(summed)
    return factors

def block_terms(scores, grade_block, weights):
    maxima, masses, counts = ([], [], [])
    for bucket in range(GRADES):
        member = grade_block == bucket
        highest = lax.optimization_barrier(jnp.max(jnp.where(member, scores, lowest), axis=1))
        masses.append(lax.optimization_barrier(jnp.sum(jnp.exp(jnp.where(member, scores - highest[:, None], lowest)), axis=1)))
        counts.append(lax.optimization_barrier(jnp.sum(member.astype(jnp.float32), axis=1)))
        maxima.append(highest)
    totals = lax.optimization_barrier(jnp.sum(scores, axis=1))
    levels = grade_levels(maxima, masses, counts)
    weighted = counts[0] * levels[0]
    for bucket in range(1, GRADES):
        weighted = weighted + counts[bucket] * levels[bucket]
    losses = (weighted - totals) / NC
    factors = slope_factors(maxima, levels, counts)
    picked_factor = jnp.zeros(scores.shape, jnp.float32)
    picked_max = jnp.zeros(scores.shape, jnp.float32)
    for bucket in range(GRADES):
        member = grade_block == bucket
        picked_factor = jnp.where(member, factors[bucket][:, None], picked_factor)
        picked_max = jnp.where(member, maxima[bucket][:, None], picked_max)
    slopes = (weights[:, None] * (picked_factor * jnp.exp(scores - picked_max) - 1.0)).astype(jnp.bfloat16)
    return (losses, slopes)

def reference(queries, candidates, grades, query_weights):
    scaling = 1.0 / math.sqrt(D)
    block_rows = math.gcd(NQ, 256)
    blocks = NQ // block_rows
    query_blocks = queries.reshape(blocks, block_rows, D)
    grade_blocks = grades.reshape(blocks, block_rows, NC)
    weight_blocks = query_weights.reshape(blocks, block_rows)

    def advance(cand_total, pieces):
        row_block, grade_block, weights = pieces
        scores = jnp.dot(row_block, candidates.T, preferred_element_type=jnp.float32) * scaling
        losses, slopes = block_terms(scores, grade_block, weights)
        query_part = (jnp.dot(slopes, candidates, preferred_element_type=jnp.float32) * scaling).astype(jnp.bfloat16)
        cand_total = cand_total + lax.dot_general(slopes, row_block, (((0,), (0,)), ((), ())), preferred_element_type=jnp.float32)
        return (cand_total, (losses, query_part))
    initial = jnp.zeros((NC, D), jnp.float32)
    final, (losses, query_parts) = lax.scan(advance, initial, (query_blocks, grade_blocks, weight_blocks))
    return (losses.reshape(NQ), query_parts.reshape(NQ, D), (final * scaling).astype(jnp.bfloat16))
```

```python
import functools
import math

import jax
import jax.numpy as jnp
from jax import lax
from jax.experimental import pallas as pl
from jax.experimental.pallas import tpu as pltpu
from jax.sharding import PartitionSpec as P

GRADES = 5
GROUPS = 1
LOWEST = -1e30
CHUNK = 64


def exchange(x, mask):
    size = lax.axis_size("col")
    return lax.ppermute(x, "col", [(i, i ^ mask) for i in range(size)])


def merge_levels(former, latter):
    top = jnp.maximum(former, latter)
    logs = top + jnp.log(jnp.exp(former - top) + jnp.exp(latter - top))
    row = lax.broadcasted_iota(jnp.int32, former.shape, former.ndim - 2)
    return jnp.where(row < GRADES, logs, former + latter)


def score_kernel(ids, q_ref, c_ref, g_ref, s_out, st_out, s_all, cols, *, scaling, rows):
    step = pl.program_id(0)

    @pl.when(step == 0)
    def _():
        s_all[...] = (
            lax.dot_general(
                q_ref[...], c_ref[...], (((1,), (1,)), ((), ())), preferred_element_type=jnp.float32
            )
            * scaling
        )

    chunk = min(CHUNK, rows)

    def body(k, _):
        at = pl.ds(pl.multiple_of(k * chunk, chunk), chunk)
        at_all = pl.ds(pl.multiple_of(step * rows + k * chunk, chunk), chunk)
        s = s_all[at_all, :]
        s_out[at, :] = s
        g = g_ref[at, :]
        lane = lax.broadcasted_iota(jnp.int32, (chunk, 128), 1)
        packed = jnp.where(lane == 2 * GRADES, jnp.sum(s, axis=1, keepdims=True), 0.0)
        members = [g == b for b in range(GRADES)]
        highest = [
            jnp.max(jnp.where(m, s, LOWEST), axis=1, keepdims=True) for m in members
        ]
        shift = jnp.broadcast_to(highest[0], s.shape)
        for b in range(1, GRADES):
            shift = jnp.where(members[b], highest[b], shift)
        e = jnp.exp(s - shift)
        for b in range(GRADES):
            mass = jnp.sum(jnp.where(members[b], e, 0.0), axis=1, keepdims=True)
            packed = jnp.where(lane == b, highest[b], packed)
            packed = jnp.where(lane == GRADES + b, mass, packed)
        cols[at_all, :] = packed
        return 0

    lax.fori_loop(0, rows // chunk, body, 0)

    @pl.when(step == pl.num_programs(0) - 1)
    def _():
        table = cols[...].T
        peak = table[0:1, :]
        summed = table[GRADES : GRADES + 1, :]
        for b in range(GRADES):
            if b:
                own = table[b : b + 1, :]
                new = jnp.maximum(peak, own)
                summed = summed * jnp.exp(peak - new) + table[
                    GRADES + b : GRADES + b + 1, :
                ] * jnp.exp(own - new)
                peak = new
            present = summed > 0.0
            st_out[b : b + 1, :] = peak + jnp.log(jnp.where(present, summed, 1.0))
        st_out[GRADES : GRADES + 1, :] = table[2 * GRADES : 2 * GRADES + 1, :]
        st_out[GRADES + 1 : 8, :] = jnp.zeros((8 - GRADES - 1, table.shape[1]), jnp.float32)


def slope_kernel(ids, s_ref, g_ref, f_ref, c_ref, slope_out, grad_out, cols, *, scaling, rows):
    step = pl.program_id(0)

    @pl.when(step == 0)
    def _():
        f = f_ref[...]
        cols[...] = jnp.concatenate([f, jnp.zeros((120, f.shape[1]), jnp.float32)], axis=0).T

    chunk = min(CHUNK, rows)

    def body(k, _):
        at = pl.ds(pl.multiple_of(k * chunk, chunk), chunk)
        at_all = pl.ds(pl.multiple_of(step * rows + k * chunk, chunk), chunk)
        s = s_ref[at, :]
        g = g_ref[at, :]
        packed = cols[at_all, :]
        shift = jnp.broadcast_to(packed[:, 0:1], s.shape)
        for b in range(1, GRADES):
            shift = jnp.where(g == b, packed[:, b : b + 1], shift)
        slope = packed[:, GRADES : GRADES + 1] * (jnp.exp(s + shift) - 1.0)
        slope_out[at_all, :] = slope.astype(jnp.bfloat16)
        return 0

    lax.fori_loop(0, rows // chunk, body, 0)

    @pl.when(step == pl.num_programs(0) - 1)
    def _():
        grad_out[...] = (
            jnp.dot(slope_out[...], c_ref[...], preferred_element_type=jnp.float32) * scaling
        ).astype(jnp.bfloat16)


def scores_of(ids, q, cand, grades, rows, scaling):
    total, width = q.shape
    columns = cand.shape[0]
    return pl.pallas_call(
        functools.partial(score_kernel, scaling=scaling, rows=rows),
        grid_spec=pltpu.PrefetchScalarGridSpec(
            num_scalar_prefetch=1,
            grid=(total // rows,),
            in_specs=[
                pl.BlockSpec((total, width), lambda i, ids: (0, 0)),
                pl.BlockSpec((columns, width), lambda i, ids: (0, 0)),
                pl.BlockSpec((rows, columns), lambda i, ids: (ids[i], 0)),
            ],
            out_specs=[
                pl.BlockSpec((rows, columns), lambda i, ids: (i, 0)),
                pl.BlockSpec((8, total), lambda i, ids: (0, 0)),
            ],
            scratch_shapes=[
                pltpu.VMEM((total, columns), jnp.float32),
                pltpu.VMEM((total, 128), jnp.float32),
            ],
        ),
        out_shape=[
            jax.ShapeDtypeStruct((total, columns), jnp.float32),
            jax.ShapeDtypeStruct((8, total), jnp.float32),
        ],
        name="scores",
    )(ids, q, cand, grades)


def slopes_of(ids, scores, grades, shifts, cand, rows, scaling):
    total, columns = scores.shape
    width = cand.shape[1]
    return pl.pallas_call(
        functools.partial(slope_kernel, scaling=scaling, rows=rows),
        grid_spec=pltpu.PrefetchScalarGridSpec(
            num_scalar_prefetch=1,
            grid=(total // rows,),
            in_specs=[
                pl.BlockSpec((rows, columns), lambda i, ids: (i, 0)),
                pl.BlockSpec((rows, columns), lambda i, ids: (ids[i], 0)),
                pl.BlockSpec((8, total), lambda i, ids: (0, 0)),
                pl.BlockSpec((columns, width), lambda i, ids: (0, 0)),
            ],
            out_specs=[
                pl.BlockSpec((total, columns), lambda i, ids: (0, 0)),
                pl.BlockSpec((total, width), lambda i, ids: (0, 0)),
            ],
            scratch_shapes=[pltpu.VMEM((total, 128), jnp.float32)],
        ),
        out_shape=[
            jax.ShapeDtypeStruct((total, columns), jnp.bfloat16),
            jax.ShapeDtypeStruct((total, width), jnp.bfloat16),
        ],
        name="slopes",
    )(ids, scores, grades, shifts, cand)


def local(queries, candidates, grades, query_weights):
    own_rows, width = queries.shape
    scaling = 1.0 / math.sqrt(width)
    col = lax.axis_size("col")
    pb = lax.axis_size("pb")
    me = lax.axis_index("col")
    me_pb = lax.axis_index("pb")
    chips = col // 2
    outer = min(4, chips)
    inner = chips // outer
    rows = own_rows // GROUPS
    piece = outer * rows
    pieces = 2 * inner
    step_z, step_y = 2 * inner, 2
    offsets = [
        [z * step_z + y * step_y + core for z in range(outer)]
        for core in range(2)
        for y in range(inner)
    ]
    flat = [o for part in offsets for o in part]
    place_of = [flat.index(o) for o in range(col)]
    holders = jnp.array(flat, jnp.int32) ^ me

    each = candidates.shape[0]
    parts = [
        (k, lax.ppermute(candidates, "pb", [((i + k) % pb, i) for i in range(pb)]))
        for k in range(1, pb)
    ]
    counts = jnp.stack([jnp.sum((grades == b).astype(jnp.float32), axis=1) for b in range(GRADES)])
    gathered = []
    for group in range(GROUPS):
        q = queries[group * rows : (group + 1) * rows]
        line = jnp.concatenate([q] + [exchange(q, z * step_z) for z in range(1, outer)], axis=0)
        line, counts = lax.optimization_barrier((line, counts))
        plane = [line] + [exchange(line, y * step_y) for y in range(1, inner)]
        gathered.append(plane)
    cand = jnp.zeros((each * pb, width), candidates.dtype)
    cand = lax.dynamic_update_slice(cand, candidates, (me_pb * each, 0))
    for k, part in parts:
        cand = lax.dynamic_update_slice(cand, part, (((me_pb + k) % pb) * each, 0))

    mask = 1
    while mask < col:
        counts = counts + exchange(counts, mask)
        mask *= 2

    def placed(x):
        k = x.shape[0]
        x = jnp.take(x.reshape(k, col, GROUPS, rows), holders, axis=1)
        x = x.reshape(k, pieces, outer, GROUPS, rows)
        return [
            x[:, :, :, group].transpose(1, 0, 2, 3).reshape(pieces, k, piece)
            for group in range(GROUPS)
        ]

    counts_of = placed(counts)
    weights_of = placed(query_weights[None])
    columns_all = grades.shape[1] * col

    losses, kept, sums, cand_total = [], [], [], None
    scored = []
    for group in range(GROUPS):
        ids = [
            (jnp.array(part, jnp.int32) ^ me) * GROUPS + group for part in offsets
        ]
        plane, done, queries_of = gathered[group], [None] * pieces, [None] * pieces
        arrived = cand
        for y in range(inner):
            for core in range(2):
                m = core * inner + y
                if core == 0:
                    q, arrived = lax.optimization_barrier((plane[y], arrived))
                    crossing = exchange(q, 1)
                else:
                    q, arrived = lax.optimization_barrier((crossing, arrived))
                queries_of[m] = q
                done[m] = scores_of(ids[m], q, cand, grades, rows, scaling)
                arrived = done[m][1]
        stats = jnp.stack([d[1] for d in done])
        for bits, size, step in ((1, 2, 1), (inner, inner, step_y), (outer, outer, step_z)):
            jump = 1
            while jump < size:
                other = exchange(stats, jump * step)
                shape = (2, inner, 8, outer, rows)
                axis = {1: 0, step_y: 1, step_z: 3}[step]
                order = [i ^ jump for i in range(size)]
                other = other.reshape(shape)
                other = jnp.concatenate(
                    [lax.slice_in_dim(other, o, o + 1, axis=axis) for o in order], axis=axis
                ).reshape(stats.shape)
                stats = merge_levels(stats, other)
                jump *= 2
        levels = [stats[:, b] for b in range(GRADES)]
        count = [counts_of[group][:, b] for b in range(GRADES)]
        weighted = count[0] * levels[0]
        for b in range(1, GRADES):
            weighted = weighted + count[b] * levels[b]
        losses.append((weighted - stats[:, GRADES]) / columns_all)
        terms = [
            jnp.where(c > 0.0, jnp.log(jnp.maximum(c, 1.0)) - lv, LOWEST)
            for c, lv in zip(count, levels)
        ]
        shifts = [None] * GRADES
        top, summed = terms[-1], jnp.ones_like(terms[-1])
        shifts[-1] = top
        for b in range(GRADES - 2, -1, -1):
            new = jnp.maximum(top, terms[b])
            summed = summed * jnp.exp(top - new) + jnp.exp(terms[b] - new)
            top = new
            shifts[b] = top + jnp.log(summed)
        zero = jnp.zeros_like(top)
        table = jnp.stack(shifts + [weights_of[group][:, 0], zero, zero], axis=1)
        slopes = [None] * pieces
        line = None
        ready = table
        for y in range(inner - 1, -1, -1):
            grads = [None, None]
            for core in (1, 0):
                m = core * inner + y
                slopes[m], grads[core] = slopes_of(
                    ids[m], done[m][0], grades, ready[m], cand, rows, scaling
                )
                ready, slopes[m], grads[core] = lax.optimization_barrier(
                    (ready, slopes[m], grads[core])
                )
                if core == 1:
                    far = exchange(grads[1], 1)
            whole = grads[0].astype(jnp.float32) + far.astype(jnp.float32)
            if y:
                sent = whole.astype(jnp.bfloat16)
                ready, sent = lax.optimization_barrier((ready, sent))
                got = exchange(sent, y * step_y)
                waiting = [got] if y == inner - 1 else waiting + [got]
            else:
                line = whole
                for got in waiting if inner > 1 else []:
                    line = line + got.astype(jnp.float32)
        total = line[:rows]
        sent = line.astype(jnp.bfloat16)
        for z in range(1, outer):
            got = exchange(sent[z * rows : (z + 1) * rows], z * step_z)
            total = total + got.astype(jnp.float32)
        sums.append(total.astype(jnp.bfloat16))
        part = lax.dot_general(
            jnp.concatenate(slopes, axis=0),
            jnp.concatenate(queries_of, axis=0),
            (((0,), (0,)), ((), ())),
            preferred_element_type=jnp.float32,
        )
        cand_total = part if cand_total is None else cand_total + part

    cand_total = cand_total * scaling
    cand_grad = lax.dynamic_slice_in_dim(cand_total, me_pb * each, each, 0)
    for k in range(1, pb):
        sent = lax.dynamic_slice_in_dim(cand_total, ((me_pb + k) % pb) * each, each, 0)
        got = lax.ppermute(
            sent.astype(jnp.bfloat16), "pb", [(i, (i + k) % pb) for i in range(pb)]
        )
        got, sums[-1] = lax.optimization_barrier((got, sums[-1]))
        cand_grad = cand_grad + got.astype(jnp.float32)

    by_place = jnp.stack([x.reshape(col, rows) for x in losses], axis=1)
    loss = jnp.take(by_place, jnp.array(place_of, jnp.int32)[jnp.arange(col) ^ me], axis=0)
    return (
        loss.reshape(col * own_rows),
        jnp.concatenate(sums, axis=0),
        cand_grad.astype(jnp.bfloat16),
    )


def solution(mesh):
    in_specs = (P(("pb", "col"), None), P(("col", "pb"), None), P("pb", "col"), P("pb"))
    out_specs = (P("pb"), P(("pb", "col"), None), P(("col", "pb"), None))
    return jax.shard_map(local, mesh=mesh, in_specs=in_specs, out_specs=out_specs, check_vma=False)
```
